256 devices in a mesh: seq: 16 (over z, core), tp: 16 (over y, x).
Axes of the slice: x: 4, y: 4, z: 8, core: 2. Of those that a mesh axis runs over, the one named last changes fastest.
Arguments:
- tokens: bfloat16 [4096, 4608], P('seq', 'tp'), may hold values from -6 to 6
- attention_gain: float32 [4608], replicated, may hold values from 0.25 to 1.75
- query_weight: bfloat16 [4608, 4096], P(None, 'tp'), may hold values from -0.09375 to 0.09375
- key_weight: bfloat16 [4608, 2048], P(None, 'tp'), may hold values from -0.09375 to 0.09375
- value_weight: bfloat16 [4608, 2048], P(None, 'tp'), may hold values from -0.09375 to 0.09375
- output_weight: bfloat16 [4096, 4608], P('tp'), may hold values from -0.09375 to 0.09375
- post_gain: float32 [4608], replicated, may hold values from 0.25 to 1.75
- local_gain: float32 [4608], replicated, may hold values from 0.25 to 1.75
- local_query_weight: bfloat16 [4608, 4096], P(None, 'tp'), may hold values from -0.09375 to 0.09375
- local_key_weight: bfloat16 [4608, 2048], P(None, 'tp'), may hold values from -0.09375 to 0.09375
- local_value_weight: bfloat16 [4608, 2048], P(None, 'tp'), may hold values from -0.09375 to 0.09375
Outputs:
- hidden: bfloat16 [4096, 4608], P('seq', 'tp')
- local_heads: bfloat16 [4096, 4096], P('seq', 'tp')
The draws below stay inside these ranges and needn't reach their ends.
All inputs are finite; a program needn't handle non-finite values.
Results may differ from the reference program's by a relative error of at most 0.02.
Values may be sent and summed in bfloat16 or wider, within the bound.
No kernel may reach another device: no remote copies, remote signals or barrier semaphores. Data moves between devices by JAX's collectives and lax.ppermute only.
A program may use at most 128 MiB of HBM per device.

```python
import jax
import jax.numpy as jnp
from jax import lax

D = 4608
HEADS = 32
KV_HEADS = 16
HEAD_DIM = 128
WINDOW = 128
TOKENS = 4096


def block_scale(stream_key, dims, shards, least, largest):
    level, own = 1.0, jax.random.fold_in(stream_key, 6)
    for dim, blocks in shards:
        heights = jnp.exp(jax.random.uniform(jax.random.fold_in(own, dim), (blocks,), jnp.float32, least / len(shards), largest / len(shards)))
        level = level * jnp.repeat(heights, dims[dim] // blocks).reshape([-1 if axis == dim else 1 for axis in range(len(dims))])
    return level


def centred(rng, dims, deviation, bound, shards=(), held_as=jnp.bfloat16):
    values = jax.random.normal(rng, dims, jnp.float32) * deviation
    if len(shards) > 0:
        values = block_scale(rng, dims, shards, -0.22, 0.18) * values
    return jnp.clip(values, min=-bound, max=bound).astype(held_as)


def setup_inputs(seed: int = 0) -> dict:
    arg_keys = jax.random.split(jax.random.key(seed), 12)
    return {
        "tokens": centred(arg_keys[0], (TOKENS, D), 1.0, 6.0, ((0, 16), (1, 16))),
        "attention_gain": jnp.clip(1.0 + 0.15 * jax.random.normal(arg_keys[1], (D,), jnp.float32), 0.25, 1.75),
        "query_weight": centred(arg_keys[2], (D, HEADS * HEAD_DIM), D ** -0.5, 0.09375, ((1, 16),)),
        "key_weight": centred(arg_keys[3], (D, KV_HEADS * HEAD_DIM), D ** -0.5, 0.09375, ((1, 16),)),
        "value_weight": centred(arg_keys[4], (D, KV_HEADS * HEAD_DIM), D ** -0.5, 0.09375, ((1, 16),)),
        "output_weight": centred(arg_keys[5], (HEADS * HEAD_DIM, D), (HEADS * HEAD_DIM) ** -0.5, 0.09375, ((0, 16),)),
        "post_gain": jnp.clip(1.0 + 0.15 * jax.random.normal(arg_keys[6], (D,), jnp.float32), 0.25, 1.75),
        "local_gain": jnp.clip(1.0 + 0.15 * jax.random.normal(arg_keys[7], (D,), jnp.float32), 0.25, 1.75),
        "local_query_weight": centred(arg_keys[8], (D, HEADS * HEAD_DIM), D ** -0.5, 0.09375, ((1, 16),)),
        "local_key_weight": centred(arg_keys[9], (D, KV_HEADS * HEAD_DIM), D ** -0.5, 0.09375, ((1, 16),)),
        "local_value_weight": centred(arg_keys[10], (D, KV_HEADS * HEAD_DIM), D ** -0.5, 0.09375, ((1, 16),)),
    }


SOFT_CAP = 50.0
NORM_EPS = 1e-06

def rms_scaled(values, weights):
    widened = values.astype(jnp.float32)
    factor = lax.rsqrt(lax.optimization_barrier(jnp.mean(widened * widened, axis=-1, keepdims=True)) + NORM_EPS)
    return widened * factor * weights.astype(jnp.float32)

def rotate(vectors, places):
    head_size = vectors.shape[-1]
    halfway = head_size // 2
    exponents = jnp.arange(halfway, dtype=jnp.float32) * (2.0 / head_size)
    frequency = jnp.power(jnp.float32(10000.0), -exponents)
    angles = places.astype(jnp.float32)[:, None] * frequency[None, :]
    cosine_part = jnp.cos(angles)[:, None, :]
    sine_part = jnp.sin(angles)[:, None, :]
    first_half = vectors[..., :halfway]
    second_half = vectors[..., halfway:]
    return jnp.concatenate([first_half * cosine_part - second_half * sine_part, second_half * cosine_part + first_half * sine_part], axis=-1)

def project_heads(normed, weight_query, weight_key, weight_value, places):
    row_count = normed.shape[0]
    queries = jnp.dot(normed, weight_query, preferred_element_type=jnp.float32).reshape(row_count, -1, HEAD_DIM)
    key_heads = jnp.dot(normed, weight_key, preferred_element_type=jnp.float32).reshape(row_count, -1, HEAD_DIM)
    value_heads = jnp.dot(normed, weight_value, preferred_element_type=jnp.float32).reshape(row_count, -1, HEAD_DIM)
    return (rotate(queries, places).astype(jnp.bfloat16), rotate(key_heads, places).astype(jnp.bfloat16), value_heads.astype(jnp.bfloat16))

def attention(queries, key_heads, value_heads, window_size):
    row_count = queries.shape[0]
    groups = HEADS // KV_HEADS
    grouped = jnp.transpose(queries.reshape(row_count, KV_HEADS, groups, HEAD_DIM), (1, 0, 2, 3))
    keys_first = jnp.transpose(key_heads, (1, 0, 2))
    values_first = jnp.transpose(value_heads, (1, 0, 2))
    places = jnp.arange(row_count, dtype=jnp.int32)
    offset = places[:, None] - places[None, :]
    allowed = (offset >= 0) & (offset < window_size)
    scale = float(D // HEADS) ** (-0.5)

    def one_head(operands):
        query_block, key_block, value_block = operands
        scores = jnp.einsum('qrd,kd->rqk', query_block.astype(jnp.float32), key_block.astype(jnp.float32)) * scale
        scores = SOFT_CAP * jnp.tanh(scores / SOFT_CAP)
        weights = jnp.where(allowed[None], jnp.exp(scores), jnp.float32(0.0))
        denominator = lax.optimization_barrier(jnp.sum(weights, axis=-1))
        probs = weights.astype(jnp.bfloat16)
        numerator = jnp.einsum('rqk,kd->qrd', probs.astype(jnp.float32), value_block.astype(jnp.float32))
        return (numerator / jnp.transpose(denominator)[:, :, None]).astype(jnp.bfloat16)
    stacked = lax.map(one_head, (grouped, keys_first, values_first))
    return jnp.transpose(stacked, (1, 0, 2, 3)).reshape(row_count, HEADS * HEAD_DIM)

def reference(tokens, attention_gain, query_weight, key_weight, value_weight, output_weight, post_gain, local_gain, local_query_weight, local_key_weight, local_value_weight):
    places = jnp.arange(TOKENS, dtype=jnp.int32)
    normed = rms_scaled(tokens, attention_gain).astype(jnp.bfloat16)
    queries, key_heads, value_heads = project_heads(normed, query_weight, key_weight, value_weight, places)
    attended = attention(queries, key_heads, value_heads, TOKENS)
    projected = jnp.dot(attended, output_weight, preferred_element_type=jnp.float32)
    hidden = (tokens.astype(jnp.float32) + rms_scaled(projected, post_gain)).astype(jnp.bfloat16)
    local_normed = rms_scaled(hidden, local_gain).astype(jnp.bfloat16)
    local_queries, local_keys, local_values = project_heads(local_normed, local_query_weight, local_key_weight, local_value_weight, places)
    local_heads = attention(local_queries, local_keys, local_values, WINDOW)
    return (hidden, local_heads)
```

```python
import functools

import jax
import jax.numpy as jnp
from jax import lax
from jax.experimental import pallas as pl
from jax.experimental.pallas import tpu as pltpu
from jax.sharding import PartitionSpec as P

D = 4608
HEADS = 32
HEAD_DIM = 128
SOFT_CAP = 50.0
NORM_EPS = 1e-06
ROWS = 256
SHARE = 288
MAIN = 256
TAIL = SHARE - MAIN
J = ("seq", "tp")
F32 = jnp.float32
BF16 = jnp.bfloat16
MIB = 1 << 20


def plane_pairs(first, shift):
    pairs = []
    for s in range(16):
        for y in range(4):
            for x in range(4):
                on_x = (s % 2 == 0) == first
                ty, tx = (y, (x + shift) % 4) if on_x else ((y + shift) % 4, x)
                pairs.append((s * 16 + y * 4 + x, s * 16 + ty * 4 + tx))
    return pairs


def seq_pairs(target):
    pairs = []
    for s in range(16):
        other = target(s)
        if 0 <= other < 16:
            pairs.extend((s * 16 + t, other * 16 + t) for t in range(16))
    return pairs


def shift_chip(array, shift):
    return lax.ppermute(array, J, seq_pairs(lambda s: (s + 2 * shift) % 16))


def swap_cores(array):
    return lax.ppermute(array, J, seq_pairs(lambda s: s ^ 1))


def vmem():
    return pl.BlockSpec(memory_space=pltpu.VMEM)


def smem():
    return pl.BlockSpec(memory_space=pltpu.SMEM)


def call(kernel, outs, *args, scalars=True, scratch=(), flops=0, limit=24, name=None):
    specs = [vmem()] * len(args)
    if scalars:
        specs[0] = smem()
    size = sum(a.size * a.dtype.itemsize for a in args)
    return pl.pallas_call(
        kernel,
        out_shape=[jax.ShapeDtypeStruct(shape, dtype) for shape, dtype in outs],
        in_specs=specs,
        out_specs=[vmem()] * len(outs),
        scratch_shapes=list(scratch),
        compiler_params=pltpu.CompilerParams(vmem_limit_bytes=limit * MIB),
        cost_estimate=pl.CostEstimate(
            flops=int(flops), bytes_accessed=int(size), transcendentals=0
        ),
        name=name,
    )(*args)


def eye(n):
    rows = lax.broadcasted_iota(jnp.int32, (n, n), 0)
    return (rows == lax.broadcasted_iota(jnp.int32, (n, n), 1)).astype(BF16)


def dot(a, b, ca=1, cb=0):
    return lax.dot_general(a, b, (((ca,), (cb,)), ((), ())), preferred_element_type=F32)


def pack_kernel(x_ref, out_ref):
    out_ref[:MAIN, :] = x_ref[:, :MAIN]
    out_ref[MAIN:, :] = dot(eye(TAIL), x_ref[:, MAIN:], 1, 1).astype(BF16)


def stack_kernel(a_ref, b_ref, c_ref, d_ref, out_ref):
    for k, ref in enumerate((a_ref, b_ref, c_ref, d_ref)):
        out_ref[k] = ref[...]


def prepare_kernel(g_ref, q_ref, k_ref, v_ref, out_ref):
    g = jnp.broadcast_to(g_ref[0], (128, 256))
    column = jnp.transpose(g)
    for j in range(2):
        out_ref[:, 128 * j : 128 * (j + 1)] = (
            q_ref[:, 128 * j : 128 * (j + 1)].astype(F32) * column
        ).astype(BF16)
    out_ref[:, 256:384] = (k_ref[...].astype(F32) * column).astype(BF16)
    out_ref[:, 384:] = (v_ref[...].astype(F32) * column).astype(BF16)


def prepare(gain, wq, wk, wv):
    steps = D // 256
    return pl.pallas_call(
        prepare_kernel,
        grid=(steps,),
        out_shape=jax.ShapeDtypeStruct((D, 512), BF16),
        in_specs=[
            pl.BlockSpec((1, 1, 256), lambda i: (i, 0, 0)),
            pl.BlockSpec((256, 256), lambda i: (i, 0)),
            pl.BlockSpec((256, 128), lambda i: (i, 0)),
            pl.BlockSpec((256, 128), lambda i: (i, 0)),
        ],
        out_specs=pl.BlockSpec((256, 512), lambda i: (i, 0)),
        compiler_params=pltpu.CompilerParams(vmem_limit_bytes=8 * MIB),
        cost_estimate=pl.CostEstimate(
            flops=4 * 10**9, bytes_accessed=D * 512 * 4, transcendentals=0
        ),
        name="prepare",
    )(gain.reshape(steps, 1, 256), wq, wk, wv)


def prepare_out_kernel(w_ref, out_ref):
    for p in range(16):
        start = SHARE * p
        low = start // 128 * 128
        high = -(-(start + SHARE) // 128) * 128
        block = w_ref[:, low:high].astype(F32)[:, start - low : start - low + SHARE]
        out_ref[:, MAIN * p : MAIN * (p + 1)] = block[:, :MAIN].astype(BF16)
        if p % 4 == 0:
            tails = []
        tails.append(block[:, MAIN:])
        if p % 4 == 3:
            at = 16 * MAIN + 128 * (p // 4)
            out_ref[:, at : at + 128] = jnp.concatenate(tails, axis=1).astype(BF16)


def block_index(pos_ref, a, b):
    return a * pos_ref[2] + b * pos_ref[3]


def lane_sums(squares):
    total = squares[:, :128]
    for j in range(1, squares.shape[1] // 128):
        total = total + squares[:, 128 * j : 128 * (j + 1)]
    return total


def gather_tails(pos_ref, x_ref, w_ref, b, wt_ref, xt_ref):
    for a in range(4):
        slot = (pos_ref[0] - a + 4) & 3
        xt_ref[TAIL * a : TAIL * (a + 1), :] = x_ref[slot, MAIN:, :]
        row = pl.multiple_of(block_index(pos_ref, a, b) * SHARE + MAIN, 16)
        wt_ref[TAIL * a : TAIL * (a + 1), :] = w_ref[pl.ds(row, TAIL), :]
    return dot(xt_ref[...], eye(128), 0, 0).astype(BF16)


def main_rows(pos_ref, w_ref, a, b):
    row = pl.multiple_of(block_index(pos_ref, a, b) * SHARE, 16)
    return w_ref[pl.ds(row, MAIN), :]


def first_kernel(shift, final, pos_ref, x_ref, w_ref, *refs):
    if shift:
        acc_ref, sq_ref, *refs = refs
    if final:
        cos_ref, sin_ref, q_ref, kv_ref, *refs = refs
    else:
        acc_out, sq_out, *refs = refs
    wt_ref, xt_ref = refs
    b = (pos_ref[1] - shift + 4) & 3
    tail = gather_tails(pos_ref, x_ref, w_ref, b, wt_ref, xt_ref)
    acc = dot(tail, wt_ref[...])
    wide = tail.astype(F32)
    sq = wide * wide
    for a in range(4):
        main = x_ref[(pos_ref[0] - a + 4) & 3, :MAIN, :]
        acc = acc + dot(main, main_rows(pos_ref, w_ref, a, b))
        wide = main.astype(F32)
        sq = sq + lane_sums(wide * wide)
    if shift:
        acc = acc + acc_ref[...]
        sq = sq + sq_ref[...]
    if final:
        factor = lax.rsqrt(jnp.sum(sq, axis=1, keepdims=True) / D + NORM_EPS)
        write_heads(acc * factor, cos_ref, sin_ref, q_ref, kv_ref)
    else:
        acc_out[...] = acc
        sq_out[...] = sq


def write_heads(u, cos_ref, sin_ref, q_ref, kv_ref):
    for j in range(3):
        head = u[:, 128 * j : 128 * (j + 1)]
        turned = head * cos_ref[...] + pltpu.roll(head, 64, 1) * sin_ref[...]
        if j < 2:
            q_ref[ROWS * j : ROWS * (j + 1), :] = turned.astype(BF16)
        else:
            kv_ref[0] = turned.astype(BF16)
    kv_ref[1] = u[:, 384:].astype(BF16)


def first_group(shift, pos, group, weights, carry, tables):
    final = tables is not None
    args = (pos, group, weights) + tuple(carry or ()) + tuple(tables or ())
    if final:
        outs = (((2 * ROWS, 128), BF16), ((2, ROWS, 128), BF16))
    else:
        outs = (((ROWS, 512), F32), ((ROWS, 128), F32))
    return call(
        functools.partial(first_kernel, shift, final),
        outs,
        *args,
        scratch=(pltpu.VMEM((128, 512), BF16), pltpu.VMEM((128, ROWS), BF16)),
        flops=2 * ROWS * 512 * D // 4,
        name="first_%d" % shift,
    )


def second_kernel(shift, final, pos_ref, y_ref, t_ref, w_ref, g_ref, gt_ref, *refs):
    if shift:
        yacc_ref, sums_ref, *refs = refs
    if final:
        tacc_ref, tsq_ref, cos_ref, sin_ref, q_ref, kv_ref, r_ref, *refs = refs
    else:
        yacc_out, sums_out, *refs = refs
    wt_ref, xt_ref = refs
    b = (pos_ref[1] - shift + 4) & 3
    ttail = gather_tails(pos_ref, t_ref, w_ref, b, wt_ref, xt_ref).astype(F32)
    tail = gather_tails(pos_ref, y_ref, w_ref, b, wt_ref, xt_ref)
    acc = dot(tail, wt_ref[...])
    wide = tail.astype(F32)
    plain = wide / gt_ref[pl.ds(pos_ref[4] * 4 + b, 1), :]
    sp, sy, sty = plain * plain, wide * wide, wide * ttail
    for a in range(4):
        slot = (pos_ref[0] - a + 4) & 3
        main = y_ref[slot, :MAIN, :]
        acc = acc + dot(main, main_rows(pos_ref, w_ref, a, b))
        wide = main.astype(F32)
        plain = wide * (1.0 / g_ref[pl.ds(block_index(pos_ref, a, b), 1), :])
        sp = sp + lane_sums(plain * plain)
        sy = sy + lane_sums(wide * wide)
        sty = sty + lane_sums(wide * t_ref[slot, :MAIN, :].astype(F32))
    if shift:
        acc = acc + yacc_ref[...]
        sp, sy, sty = sp + sums_ref[0], sy + sums_ref[1], sty + sums_ref[2]
    if final:
        sp, sy, sty, st = (
            jnp.sum(s, axis=1, keepdims=True) for s in (sp, sy, sty, tsq_ref[...])
        )
        r = lax.rsqrt(sp / D + NORM_EPS)
        mean = jnp.maximum(st + 2.0 * r * sty + r * r * sy, 0.0) / D
        factor = lax.rsqrt(mean + NORM_EPS)
        write_heads((tacc_ref[...] + acc * r) * factor, cos_ref, sin_ref, q_ref, kv_ref)
        r_ref[...] = jnp.broadcast_to(r, (ROWS, 128))
    else:
        yacc_out[...] = acc
        sums_out[0], sums_out[1], sums_out[2] = sp, sy, sty


def second_group(shift, pos, group, tokens_group, weights, gains, carry, last):
    final = last is not None
    args = (pos, group, tokens_group, weights) + tuple(gains) + tuple(carry or ())
    args += tuple(last or ())
    if final:
        outs = (
            ((2 * ROWS, 128), BF16),
            ((2, ROWS, 128), BF16),
            ((ROWS, 128), F32),
        )
    else:
        outs = (((ROWS, 512), F32), ((3, ROWS, 128), F32))
    return call(
        functools.partial(second_kernel, shift, final),
        outs,
        *args,
        scratch=(pltpu.VMEM((128, 512), BF16), pltpu.VMEM((128, ROWS), BF16)),
        flops=2 * ROWS * 512 * D // 4,
        name="second_%d" % shift,
    )


def weigh(queries, keys):
    scores = dot(queries, keys, 1, 1) * (1.0 / (SOFT_CAP * 12.0))
    return jnp.exp(SOFT_CAP * jnp.tanh(scores))


def own_kernel(pos_ref, q_ref, other_ref, kv_ref, num_ref, den_ref):
    rows = lax.broadcasted_iota(jnp.int32, (ROWS, ROWS), 0)
    columns = lax.broadcasted_iota(jnp.int32, (ROWS, ROWS), 1)
    keys, values = kv_ref[0], kv_ref[1]
    full = jnp.where(pos_ref[4] == 0, 1.0, 0.0).astype(F32)
    for j in range(4):
        ref = q_ref if j < 2 else other_ref
        w = weigh(ref[ROWS * (j % 2) : ROWS * (j % 2 + 1), :], keys)
        if j < 2:
            w = jnp.where(rows >= columns, w, 0.0)
        else:
            w = w * full
        den_ref[ROWS * j : ROWS * (j + 1), :] = lane_sums(w)
        num_ref[ROWS * j : ROWS * (j + 1), :] = dot(w.astype(BF16), values)


def more_kernel(offsets, split, pos_ref, q_ref, other_ref, num_in, den_in, *refs):
    kv_refs, outs = refs[: len(offsets)], refs[len(offsets) :]
    if split:
        mine_ref, theirs_ref = outs
        num_ref, den_ref = None, None
    else:
        num_ref, den_ref = outs
    chip = pos_ref[5]

    def target(which, j):
        if split:
            ref = mine_ref if j < 2 else theirs_ref
            return ref.at[which, pl.ds(ROWS * (j % 2), ROWS), :]
        ref = (num_ref, den_ref)[which]
        return ref.at[pl.ds(ROWS * j, ROWS), :]

    for j in range(4):
        span = pl.ds(ROWS * j, ROWS)
        target(0, j)[...] = num_in[span, :]
        target(1, j)[...] = den_in[span, :]
    for offset, kv_ref in zip(offsets, kv_refs):
        source = (chip - offset + 8) & 7

        @pl.when(source < chip)
        def _(kv_ref=kv_ref):
            keys, values = kv_ref[0], kv_ref[1]
            for j in range(4):
                ref = q_ref if j < 2 else other_ref
                w = weigh(ref[ROWS * (j % 2) : ROWS * (j % 2 + 1), :], keys)
                den, num = target(1, j), target(0, j)
                den[...] += lane_sums(w)
                num[...] += dot(w.astype(BF16), values)


def project_kernel(pos_ref, mine_ref, theirs_ref, w_ref, *refs):
    out_refs, tails = refs[:4], refs[4]
    total = mine_ref[...] + theirs_ref[...]
    heads = []
    for j in range(2):
        den = jnp.sum(total[1, ROWS * j : ROWS * (j + 1), :], axis=1, keepdims=True)
        heads.append((total[0, ROWS * j : ROWS * (j + 1), :] / den).astype(BF16))
    attended = jnp.concatenate(heads, axis=1)
    tails[...] = dot(w_ref[:, 16 * MAIN :], attended, 0, 1).astype(BF16)
    for k in (2, 1, 3, 0):
        b = (pos_ref[1] + k) & 3
        for a in range(4):
            p = block_index(pos_ref, a, b)
            w = w_ref[:, pl.ds(pl.multiple_of(p * MAIN, MAIN), MAIN)]
            out_refs[k][a, :MAIN, :] = dot(attended, w).astype(BF16)
            row = pl.multiple_of(p * TAIL, TAIL)
            out_refs[k][a, MAIN:, :] = tails[pl.ds(row, TAIL), :]


def reduce_kernel(pos_ref, a_ref, b_ref, c_ref, d_ref, *out_refs):
    for k in range(4):
        a = (pos_ref[0] + k) & 3
        total = a_ref[a].astype(F32) + b_ref[a].astype(F32)
        total = total + c_ref[a].astype(F32) + d_ref[a].astype(F32)
        out_refs[k][...] = total.astype(out_refs[k].dtype)


def finish_kernel(pos_ref, own_ref, b_ref, c_ref, d_ref, g_ref, gt_ref, out_ref):
    total = own_ref[...] + b_ref[...].astype(F32) + c_ref[...].astype(F32)
    total = total + d_ref[...].astype(F32)
    p = pos_ref[6]
    out_ref[:MAIN, :] = (total[:MAIN] * g_ref[pl.ds(p, 1), :]).astype(BF16)
    tail_gain = gt_ref[pl.ds(pos_ref[4] * 4 + pos_ref[1], 1), :]
    column = jnp.transpose(jnp.broadcast_to(tail_gain, (128, 128)))
    for a in range(4):

        @pl.when(pos_ref[0] == a)
        def _(a=a):
            gain = column[TAIL * a : TAIL * (a + 1), :]
            for j in range(2):
                out_ref[MAIN:, 128 * j : 128 * (j + 1)] = (
                    total[MAIN:, 128 * j : 128 * (j + 1)] * gain
                ).astype(BF16)


def hidden_kernel(x_ref, y_ref, r_ref, out_ref):
    r = r_ref[...]
    for j in range(2):
        span = slice(128 * j, 128 * (j + 1))
        out_ref[:, span] = (
            x_ref[:, span].astype(F32) + r * y_ref[:MAIN, span].astype(F32)
        ).astype(BF16)
    tail = dot(y_ref[MAIN:, :], eye(TAIL), 0, 0)
    out_ref[:, MAIN:] = (x_ref[:, MAIN:].astype(F32) + r[:, :TAIL] * tail).astype(BF16)


def window_kernel(q_ref, kv_ref, num_ref, den_ref):
    rows = lax.broadcasted_iota(jnp.int32, (ROWS, ROWS), 0)
    columns = lax.broadcasted_iota(jnp.int32, (ROWS, ROWS), 1)
    allowed = (rows >= columns) & (rows - columns < 128)
    for j in range(2):
        span = slice(ROWS * j, ROWS * (j + 1))
        w = jnp.where(allowed, weigh(q_ref[span, :], kv_ref[0]), 0.0)
        den_ref[span, :] = lane_sums(w)
        num_ref[span, :] = dot(w.astype(BF16), kv_ref[1])


def halo_kernel(pos_ref, q_ref, kv_ref, num_ref, den_ref, out_ref):
    rows = lax.broadcasted_iota(jnp.int32, (128, 128), 0)
    columns = lax.broadcasted_iota(jnp.int32, (128, 128), 1)
    allowed = (columns > rows) & (pos_ref[5] * 2 + pos_ref[4] > 0)
    for j in range(2):
        at = ROWS * j
        w = jnp.where(allowed, weigh(q_ref[at : at + 128, :], kv_ref[0]), 0.0)
        num = num_ref[at : at + 128, :] + dot(w.astype(BF16), kv_ref[1])
        den = jnp.sum(den_ref[at : at + 128, :] + w, axis=1, keepdims=True)
        out_ref[:128, 128 * j : 128 * (j + 1)] = (num / den).astype(BF16)
        den = jnp.sum(den_ref[at + 128 : at + 256, :], axis=1, keepdims=True)
        out_ref[128:, 128 * j : 128 * (j + 1)] = (
            num_ref[at + 128 : at + 256, :] / den
        ).astype(BF16)


def gather_plane(own):
    near = {d: lax.ppermute(own, J, plane_pairs(True, d)) for d in (2, 1, 3)}
    (group,) = call(
        stack_kernel,
        (((4, SHARE, ROWS), BF16),),
        own,
        near[1],
        near[2],
        near[3],
        scalars=False,
        flops=10**8,
        name="stack",
    )
    far = {d: lax.ppermute(group, J, plane_pairs(False, d)) for d in (2, 1, 3)}
    return {0: group, **far}


def local(
    tokens,
    attention_gain,
    query_weight,
    key_weight,
    value_weight,
    output_weight,
    post_gain,
    local_gain,
    local_query_weight,
    local_key_weight,
    local_value_weight,
):
    section = lax.axis_index("seq")
    head = lax.axis_index("tp")
    core, chip = section % 2, section // 2
    y, x = head // 4, head % 4
    swap = core == 1
    pos = jnp.stack(
        [
            jnp.where(swap, y, x),
            jnp.where(swap, x, y),
            jnp.where(swap, 4, 1),
            jnp.where(swap, 1, 4),
            core,
            chip,
            head,
        ]
    ).astype(jnp.int32)

    halfway = HEAD_DIM // 2
    exponents = jnp.arange(halfway, dtype=F32) * (2.0 / HEAD_DIM)
    frequency = jnp.power(F32(10000.0), -exponents)
    places = section * ROWS + lax.iota(jnp.int32, ROWS)
    angles = places.astype(F32)[:, None] * frequency[None, :]
    cosine, sine = jnp.cos(angles), jnp.sin(angles)
    tables = (
        jnp.concatenate([cosine, cosine], axis=1),
        jnp.concatenate([-sine, sine], axis=1),
    )

    (own,) = call(
        pack_kernel,
        (((SHARE, ROWS), BF16),),
        tokens,
        scalars=False,
        flops=10**8,
        name="pack",
    )
    first_weights = prepare(attention_gain, query_weight, key_weight, value_weight)
    groups = gather_plane(own)
    second_weights = prepare(
        local_gain, local_query_weight, local_key_weight, local_value_weight
    )
    (out_weights,) = call(
        prepare_out_kernel,
        (((ROWS, D), BF16),),
        output_weight,
        scalars=False,
        flops=4 * 10**9,
        name="prepare_out",
    )
    by_block = post_gain.reshape(16, SHARE)
    tail_gain = by_block[:, MAIN:].reshape(4, 4, TAIL)
    gains = (
        by_block[:, :MAIN],
        jnp.concatenate(
            [tail_gain.reshape(4, 128), jnp.swapaxes(tail_gain, 0, 1).reshape(4, 128)]
        ),
    )

    carry = None
    for d in (0, 1, 3):
        carry = first_group(d, pos, groups[d], first_weights, carry, None)
    queries, kv = first_group(2, pos, groups[2], first_weights, carry, tables)

    blocks = {d: shift_chip(kv, d) for d in (2, -2, 1, -1)}
    others = swap_cores(queries)
    score_flops = 4 * 4 * ROWS * ROWS * 128 * 4
    state = ((4 * ROWS, 128), F32)
    num, den = call(
        own_kernel, (state, state), pos, queries, others, kv, flops=score_flops, name="own"
    )
    half_up = shift_chip(blocks[2][:, :128], 2)
    half_down = shift_chip(blocks[-2][:, 128:], -2)
    blocks[3] = shift_chip(blocks[2], 1)
    blocks[-3] = shift_chip(blocks[-2], -1)
    num, den = call(
        functools.partial(more_kernel, (1, -1, 2, -2), False),
        (state, state),
        pos,
        queries,
        others,
        num,
        den,
        blocks[1],
        blocks[-1],
        blocks[2],
        blocks[-2],
        flops=4 * score_flops,
        name="more",
    )
    part = ((2, 2 * ROWS, 128), F32)
    mine, theirs = call(
        functools.partial(more_kernel, (3, -3, 4, 4), True),
        (part, part),
        pos,
        queries,
        others,
        num,
        den,
        blocks[3],
        blocks[-3],
        half_up,
        half_down,
        flops=3 * score_flops,
        name="last",
    )
    received = swap_cores(theirs)

    carry = None
    for d in (0, 1, 3, 2):
        carry = first_group(d, pos, groups[d], second_weights, carry, None)
    tokens_acc, tokens_sq = carry

    chunk = ((4, SHARE, ROWS), BF16)
    chunks = call(
        project_kernel,
        (chunk,) * 4,
        pos,
        mine,
        received,
        out_weights,
        scratch=(pltpu.VMEM((16 * TAIL, ROWS), BF16),),
        flops=2 * ROWS * ROWS * D,
        name="project",
    )
    arrived = {d: lax.ppermute(chunks[d], J, plane_pairs(False, d)) for d in (2, 1, 3)}
    block = ((SHARE, ROWS), BF16)
    pieces = call(
        reduce_kernel,
        (((SHARE, ROWS), F32), block, block, block),
        pos,
        chunks[0],
        arrived[1],
        arrived[2],
        arrived[3],
        flops=10**8,
        name="reduce",
    )
    arrived = {d: lax.ppermute(pieces[d], J, plane_pairs(True, d)) for d in (2, 1, 3)}
    (scaled,) = call(
        finish_kernel,
        (block,),
        pos,
        pieces[0],
        arrived[1],
        arrived[2],
        arrived[3],
        *gains,
        flops=10**8,
        name="finish",
    )
    rows = gather_plane(scaled)
    carry = None
    for d in (0, 1, 3):
        carry = second_group(d, pos, rows[d], groups[d], second_weights, gains, carry, None)
    queries, kv, r = second_group(
        2,
        pos,
        rows[2],
        groups[2],
        second_weights,
        gains,
        carry,
        (tokens_acc, tokens_sq) + tables,
    )

    edge = lax.ppermute(kv[:, 128:], J, seq_pairs(lambda s: s + 1))
    state = ((2 * ROWS, 128), F32)
    num, den = call(
        window_kernel,
        (state, state),
        queries,
        kv,
        scalars=False,
        flops=score_flops // 2,
        name="window",
    )
    (hidden,) = call(
        hidden_kernel,
        (((ROWS, SHARE), BF16),),
        tokens,
        scaled,
        r,
        scalars=False,
        flops=10**8,
        name="hidden",
    )
    (local_heads,) = call(
        halo_kernel,
        (((ROWS, 256), BF16),),
        pos,
        queries,
        edge,
        num,
        den,
        flops=score_flops // 8,
        name="halo",
    )
    return hidden, local_heads


def solution(mesh):
    in_specs = (
        P("seq", "tp"),
        P(),
        P(None, "tp"),
        P(None, "tp"),
        P(None, "tp"),
        P("tp", None),
        P(),
        P(),
        P(None, "tp"),
        P(None, "tp"),
        P(None, "tp"),
    )
    out_specs = (P("seq", "tp"), P("seq", "tp"))
    return jax.shard_map(local, mesh=mesh, in_specs=in_specs, out_specs=out_specs, check_vma=False)
```
